32 devices in a mesh: section: 2 (over y), ep: 16 (over z, x, core).
Axes of the slice: x: 2, y: 2, z: 4, core: 2. Of those that a mesh axis runs over, the one named last changes fastest.
Arguments:
- inputs: bfloat16 [2, 2048, 1536], P('section', 'ep'), may hold values from -6 to 6
- upstream: bfloat16 [2, 2048, 1536], P('section', 'ep'), may hold values from -6 to 6
- gate_saved: bfloat16 [2, 2048, 8, 384], P('section', 'ep'), may hold values from -6 to 6
- expert_ids: int32 [2, 2048, 8], P('section', 'ep'), may hold values from 0 to 31, all different within a row; in each aligned block of 128 rows (0 to 127, 128 to 255, ..., all dimensions but the last counted through in order) at most 48 rows name the same one
- route_weights: float32 [2, 2048, 8], P('section', 'ep'), may hold values from 0.05 to 0.5
- w_up: bfloat16 [2, 32, 1536, 384], P('section', 'ep'), may hold values from -0.15625 to 0.15625
- w_down: bfloat16 [2, 32, 384, 1536], P('section', 'ep'), may hold values from -0.3125 to 0.3125
Outputs:
- delivered: bfloat16 [2, 2048, 1536], P('section', 'ep')
- grad_up: bfloat16 [2, 32, 1536, 384], P('section', 'ep')
- grad_down: bfloat16 [2, 32, 384, 1536], P('section', 'ep')
The draws below stay inside these ranges and needn't reach their ends.
Inputs may be any that keep to these rules, and one draw needn't show every extreme that they name: `expert_ids`: each row names 8 different experts. In the rows of one device no expert is named more than 48 times, and in every draw some expert is named exactly 48 times in the rows of some device; every expert is named somewhere.
All inputs are finite; a program needn't handle non-finite values.
Results may differ from the reference program's by a relative error of at most 0.012.
Values may be sent and summed in bfloat16 or wider, within the bound.
A program may use at most 192 MiB of HBM per device.

```python
import math
import jax
import jax.numpy as jnp
import numpy as np
from jax import lax

D = 1536
FF = 384
TOP = 8
TOK_DEV = 128
EXPERTS = 32
TOKENS = 2048
CAP = 48
N_SECTION = 2
N_EP = 16


def level_of(stream_key, shape, split, least, high):
    loudness, own = 1.0, jax.random.fold_in(stream_key, 6)
    for dim, parts in split:
        heights = jnp.exp(jax.random.uniform(jax.random.fold_in(own, dim), (parts,), jnp.float32, least / len(split), high / len(split)))
        loudness = loudness * jnp.repeat(heights, shape[dim] // parts).reshape([-1 if axis == dim else 1 for axis in range(len(shape))])
    return loudness


def assign_block(key, own, number, rows, amount, top, most, skew):
    order = jax.random.permutation(key, amount)
    packed, common = load_shares(amount, rows * top, most, skew, True), load_shares(amount, rows * top, most, skew, False)
    places = jnp.arange(amount)

    def named(sizes, rotation):
        used = int((sizes > 0).sum())
        fixed = max(1, used // 4)
        shifted = fixed + (places - fixed + rotation * (used - fixed)) % max(1, amount - fixed)
        return jnp.zeros((amount,), jnp.int32).at[order[jnp.where(places < fixed, places, shifted)]].set(jnp.asarray(sizes, jnp.int32))

    sizes = jnp.where(number % 4 == 0, named(packed, number // 4), named(common, number - number // 4 - 1))
    mixed = jax.random.permutation(jax.random.fold_in(own, 3), amount)
    donor, taker = mixed[0:amount // 2 * 2:2], mixed[1:amount // 2 * 2:2]
    slack = jnp.minimum(sizes[donor] - 1, most - sizes[taker]) // 2
    slack = jnp.where((donor == order[0]) | (taker == order[0]) | (sizes[taker] == 0), 0, jnp.maximum(slack, 0))
    shifted = jax.random.randint(jax.random.fold_in(own, 4), (amount // 2,), 0, 1 << 20) % (slack + 1)
    sizes = sizes.at[donor].add(-shifted).at[taker].add(shifted)
    labels = jnp.searchsorted(jnp.cumsum(sizes), jnp.arange(rows * top), side="right").astype(jnp.int32)
    table = labels.reshape(top, rows).T
    table = table[jax.random.permutation(jax.random.fold_in(own, 1), rows)]
    rotation = jax.random.randint(jax.random.fold_in(own, 2), (rows, 1), 0, top)
    return jnp.take_along_axis(table, (jnp.arange(top)[None, :] + rotation) % top, axis=1)


def load_shares(amount, total, most, slope, full):
    portions = [(1 << 20) // math.isqrt(rank ** slope) + 1 for rank in range(1, amount + 1)]
    largest = most if full else min(most, max(-(-total // amount), total * portions[0] // sum(portions)))
    least = 1 if total - largest >= amount - 1 else 0
    holding, surplus = [largest] + [least] * (amount - 1), total - largest - least * (amount - 1)
    while surplus > 0:
        free = [i for i in range(1, amount) if holding[i] < largest] or [i for i in range(1, amount) if holding[i] < most]
        whole, left = sum([portions[i] for i in free]), surplus
        for i in free:
            extra = min(most - holding[i], max(1, left * portions[i] // whole), surplus)
            holding[i] = holding[i] + extra
            surplus = surplus - extra
    return np.array(holding)


def gaussian(key, dims, deviation, limit, cuts=(), kind=jnp.bfloat16):
    result = jax.random.normal(key, dims, jnp.float32) * deviation
    if len(cuts) > 0:
        result = level_of(key, dims, cuts, -0.22, 0.18) * result
    return jnp.clip(result, min=-limit, max=limit).astype(kind)


def setup_inputs(seed: int = 0) -> dict:
    arg_keys = jax.random.split(jax.random.key(seed), 8)
    inputs = gaussian(arg_keys[0], (N_SECTION, TOKENS, D), 1.0, 6.0, ((0, 2), (1, 16)))
    upstream = gaussian(arg_keys[1], (N_SECTION, TOKENS, D), 1.0, 6.0, ((0, 2), (1, 16)))
    gate_saved = gaussian(arg_keys[2], (N_SECTION, TOKENS, TOP, FF), 1.5, 6.0, ((0, 2), (1, 16)))
    expert_ids_keys = jax.random.split(jax.random.fold_in(arg_keys[3], 1), N_SECTION * TOKENS // TOK_DEV)
    expert_ids_turns = jax.random.permutation(jax.random.fold_in(arg_keys[3], 3), N_SECTION * TOKENS // TOK_DEV)
    expert_ids = jax.vmap(lambda own, number: assign_block(jax.random.fold_in(arg_keys[3], 2), own, number, TOK_DEV, EXPERTS, TOP, CAP, 2))(expert_ids_keys, expert_ids_turns).reshape((N_SECTION, TOKENS, TOP))
    route_weights = jnp.clip(jnp.exp(math.log(0.5) - 2.3025851 * jax.random.uniform(arg_keys[4], (N_SECTION, TOKENS, TOP), jnp.float32) ** level_of(arg_keys[4], (N_SECTION, TOKENS, TOP), ((0, 2), (1, 16)), -0.2, 0.2)), 0.05, 0.5)
    w_up = gaussian(arg_keys[5], (N_SECTION, EXPERTS, D, FF), D ** -0.5, 0.15625, ((0, 2), (1, 16)))
    w_down = gaussian(arg_keys[6], (N_SECTION, EXPERTS, FF, D), FF ** -0.5, 0.3125, ((0, 2), (1, 16)))
    return {"inputs": inputs, "upstream": upstream, "gate_saved": gate_saved, "expert_ids": expert_ids, "route_weights": route_weights, "w_up": w_up, "w_down": w_down}


def one_section(operands):
    tokens_here, cotangent, gate_layer, id_layer, weight_layer, up_layer, down_layer = operands
    rows_block = TOK_DEV * TOP
    flat_ids = id_layer.reshape(N_EP, rows_block)
    onehot = (flat_ids[:, :, None] == jnp.arange(EXPERTS, dtype=jnp.int32)[None, None, :]).astype(jnp.int32)
    position = jnp.sum(jnp.cumsum(onehot, axis=1) * onehot, axis=2) - 1
    sources = jnp.arange(N_EP, dtype=jnp.int32)[:, None]
    slot_index = (sources * CAP + position).astype(jnp.int32)
    flat_index = jnp.arange(N_EP * rows_block, dtype=jnp.int32).reshape(N_EP, rows_block)
    table = jnp.full((EXPERTS, N_EP * CAP), N_EP * rows_block, jnp.int32)
    table = table.at[flat_ids, slot_index].set(flat_index)
    gate_flat = gate_layer.reshape(TOKENS * TOP, FF)
    weight_flat = weight_layer.reshape(TOKENS * TOP)

    def per_expert(carry, expert_args):
        slot_rows, up_weight, down_weight = expert_args
        token_of = (slot_rows // TOP).astype(jnp.int32)
        x_rows = jnp.take(tokens_here, token_of, axis=0, mode="fill", fill_value=0)
        gate_rows = jnp.take(gate_flat, slot_rows, axis=0, mode="fill", fill_value=0)
        scale_rows = jnp.take(weight_flat, slot_rows, axis=0, mode="fill", fill_value=0)
        cot_rows = jnp.take(cotangent, token_of, axis=0, mode="fill", fill_value=0)
        scaled = (scale_rows[:, None] * cot_rows.astype(jnp.float32)).astype(jnp.bfloat16)
        activation = jax.nn.silu(gate_rows.astype(jnp.float32))
        up_value = jnp.dot(x_rows, up_weight, preferred_element_type=jnp.float32)
        hidden = (activation * up_value).astype(jnp.bfloat16)
        grad_down = jnp.dot(hidden.T, scaled, preferred_element_type=jnp.float32)
        grad_hidden = jnp.dot(scaled, down_weight.T, preferred_element_type=jnp.float32)
        grad_rows = (grad_hidden * activation).astype(jnp.bfloat16)
        grad_up = jnp.dot(x_rows.T, grad_rows, preferred_element_type=jnp.float32)
        slot_grad = jnp.dot(grad_rows, up_weight.T, preferred_element_type=jnp.float32).astype(jnp.bfloat16)
        carry = carry.at[token_of].add(slot_grad.astype(jnp.float32), mode="drop")
        return carry, (grad_up.astype(jnp.bfloat16), grad_down.astype(jnp.bfloat16))

    start = jnp.zeros((TOKENS, D), jnp.float32)
    layer_grad, grads = lax.scan(per_expert, start, (table, up_layer, down_layer))
    return layer_grad.astype(jnp.bfloat16), grads[0], grads[1]


def reference(inputs, upstream, gate_saved, expert_ids, route_weights, w_up, w_down):
    cot_all = jnp.roll(upstream, -1, axis=0)
    layer_grads, grad_up, grad_down = lax.map(one_section, (inputs, cot_all, gate_saved, expert_ids, route_weights, w_up, w_down))
    delivered = jnp.roll(layer_grads, -1, axis=0)
    return delivered, grad_up, grad_down
```

```python
import jax
import jax.numpy as jnp
from jax import lax
from jax.sharding import PartitionSpec as P

BF16 = jnp.bfloat16
F32 = jnp.float32


def from_behind(block, axis, distance):
    devices = range(lax.axis_size(axis))
    route = [((i - distance) % len(devices), i) for i in devices]
    return lax.ppermute(block, axis, route)


def body(inputs, upstream, gate_saved, expert_ids, route_weights, w_up, w_down):
    ep = lax.axis_size("ep")
    local = w_up.shape[1]
    experts = local * ep
    toks, top = expert_ids.shape[1:]
    cap = 3 * toks * top // (2 * experts)
    width = inputs.shape[2]
    ff = w_up.shape[3]

    routing = jnp.concatenate([expert_ids[0].astype(F32), route_weights[0]], axis=1)
    routing_all = lax.all_gather(routing, "ep", axis=0, tiled=False)

    ids = expert_ids[0]
    hit = ids[:, :, None] == jnp.arange(experts, dtype=jnp.int32)
    member = jnp.any(hit, axis=1).astype(BF16)
    lower = (jnp.arange(toks)[:, None] > jnp.arange(toks)[None, :]).astype(BF16)
    rank = jnp.dot(lower, member, preferred_element_type=F32)
    place = jnp.sum(jnp.where(hit, rank[:, None, :], 0.0), axis=2)
    slot = (ids * cap + place.astype(jnp.int32)).reshape(1, toks * top)
    pick = (jnp.arange(experts * cap, dtype=jnp.int32)[:, None] == slot).astype(BF16)
    gate_send = jnp.dot(pick, gate_saved[0].reshape(toks * top, ff), preferred_element_type=F32)
    gate_send = gate_send.astype(BF16).reshape(ep, local, cap, ff)
    gate_recv = lax.all_to_all(gate_send, "ep", split_axis=0, concat_axis=0, tiled=True)

    cot = from_behind(upstream, "section", -1)[0]
    x_all = lax.all_gather(inputs[0], "ep", axis=0, tiled=True)
    c_all = lax.all_gather(cot, "ep", axis=0, tiled=True)

    me = lax.axis_index("ep")
    mine = (me * local + jnp.arange(local)).astype(F32)
    hits = routing_all[:, :, :top, None] == mine
    weight = jnp.sum(jnp.where(hits, routing_all[:, :, top:, None], 0.0), axis=2)
    members = jnp.any(hits, axis=2)
    ranks = jnp.einsum("ab,sbe->sae", lower, members.astype(BF16), preferred_element_type=F32)
    ranks = jnp.where(members, ranks, -1.0)
    spread = (ranks[:, :, :, None] == jnp.arange(cap).astype(F32)).astype(BF16)
    gate = jnp.einsum("stec,secf->stef", spread, gate_recv, preferred_element_type=F32)
    act = jax.nn.silu(gate).reshape(ep * toks, local, ff)
    weight = weight.reshape(ep * toks, local, 1)
    act_w = (act * weight)

    up = w_up[0]
    down = w_down[0]
    up_cat = jnp.transpose(up, (1, 0, 2)).reshape(width, local * ff)
    down_cat = down.reshape(local * ff, width)
    act_w = act_w.reshape(ep * toks, local * ff)
    u = jnp.dot(x_all, up_cat, preferred_element_type=F32)
    hidden = (act_w * u).astype(BF16)
    h = lax.dot_general(c_all, down_cat, (((1,), (1,)), ((), ())), preferred_element_type=F32)
    g = (act_w * h).astype(BF16)
    part = lax.dot_general(g, up_cat, (((1,), (1,)), ((), ())), preferred_element_type=F32)
    grad = lax.psum_scatter(part.astype(BF16), "ep", scatter_dimension=0, tiled=True)
    delivered = from_behind(grad[None], "section", -1)
    grad_down = lax.dot_general(hidden, c_all, (((0,), (0,)), ((), ())), preferred_element_type=F32)
    grad_up = jnp.stack([
        lax.dot_general(x_all, g[:, e * ff:(e + 1) * ff], (((0,), (0,)), ((), ())), preferred_element_type=F32)
        for e in range(local)
    ])
    return (
        delivered,
        grad_up.astype(BF16)[None],
        grad_down.astype(BF16).reshape(1, local, ff, width),
    )


def solution(mesh):
    return jax.shard_map(
        body,
        mesh=mesh,
        in_specs=(
            P("section", "ep", None),
            P("section", "ep", None),
            P("section", "ep", None, None),
            P("section", "ep", None),
            P("section", "ep", None),
            P("section", "ep", None, None),
            P("section", "ep", None, None),
        ),
        out_specs=(
            P("section", "ep", None),
            P("section", "ep", None, None),
            P("section", "ep", None, None),
        ),
        check_vma=False,
    )
```

```python
import functools

import jax
import jax.numpy as jnp
from jax import lax
from jax.experimental import pallas as pl
from jax.experimental.pallas import tpu as pltpu
from jax.sharding import PartitionSpec as P

BF16 = jnp.bfloat16
F32 = jnp.float32


def from_behind(block, axis, distance):
    devices = range(lax.axis_size(axis))
    route = [((i - distance) % len(devices), i) for i in devices]
    return lax.ppermute(block, axis, route)


def gather_kernel(grid, sections, x_ref, u_ref, x_out, c_out, own_sem, shift_send, send_sem, recv_sem, pair_recv):
    outer, inner, pair = grid
    me = lax.axis_index("ep")
    sec = lax.axis_index("section")
    core = lax.rem(me, pair)
    here = (lax.div(me, inner * pair), lax.rem(lax.div(me, pair), inner))
    sizes = (outer, inner)
    half = x_ref.shape[0] // 2

    def moved(dim, step):
        spot = list(here)
        spot[dim] = lax.rem(here[dim] + step + sizes[dim], sizes[dim])
        return (spot[0] * inner + spot[1]) * pair + core

    other = me + 1 - 2 * core
    before = lax.rem(sec + sections - 1, sections)
    after = lax.rem(sec + 1, sections)

    barrier = pltpu.get_barrier_semaphore()
    greeted = 0
    for target in [{"section": before}, {"section": after}] + [
        {"ep": d} for d in [other] + [moved(dim, step) for dim in range(2) if sizes[dim] > 1 for step in (1, -1)]
    ]:
        pl.semaphore_signal(barrier, inc=1, device_id=target, device_id_type=pl.DeviceIdType.MESH)
        greeted += 1
    pl.semaphore_wait(barrier, greeted)

    outs = (x_out, c_out)
    orders = ((0, 1), (1, 0))
    pending = []

    def slice_of(a, owner, h):
        return outs[a].at[owner, pl.ds(h * half, half)]

    def own_slice(ref, h):
        return ref.at[pl.ds(h * half, half)]

    for h in range(2):
        cp = pltpu.make_async_remote_copy(
            src_ref=own_slice(u_ref, h), dst_ref=slice_of(1, me, h),
            send_sem=shift_send.at[h], recv_sem=recv_sem.at[1, 0, h],
            device_id={"section": before}, device_id_type=pl.DeviceIdType.MESH)
        cp.start()
        pending.append(cp)
    keep = pltpu.make_async_copy(x_ref, x_out.at[me], own_sem)
    keep.start()

    arrivals = []
    for level in range(outer + inner - 1):
        for a in range(2):
            d1, d2 = orders[a]
            for i in range(sizes[d1]):
                j = level - i
                if j < 0 or j >= sizes[d2]:
                    continue
                for h in range(2):
                    sign = 1 - 2 * h
                    spot = [None, None]
                    spot[d1] = lax.rem(here[d1] - sign * i + sizes[d1], sizes[d1])
                    spot[d2] = lax.rem(here[d2] - sign * j + sizes[d2], sizes[d2])
                    base = (spot[0] * inner + spot[1]) * pair
                    owner = base + core
                    n = i * sizes[d2] + j
                    block = slice_of(a, owner, h)
                    if a == 1 or level > 0:
                        pltpu.make_async_remote_copy(
                            src_ref=block, dst_ref=block, send_sem=send_sem.at[a, n, h, 0],
                            recv_sem=recv_sem.at[a, n, h], device_id={"ep": other},
                            device_id_type=pl.DeviceIdType.MESH).wait_recv()
                    src = own_slice(x_ref, h) if (a == 0 and level == 0) else block
                    hops = []
                    if j == 0 and i < sizes[d1] - 1:
                        hops.append((1, moved(d1, sign), recv_sem.at[a, (i + 1) * sizes[d2], h]))
                    if j < sizes[d2] - 1:
                        hops.append((2, moved(d2, sign), recv_sem.at[a, n + 1, h]))
                    hops.append((0, other, pair_recv.at[a, n, h]))
                    for kind, target, landed in hops:
                        cp = pltpu.make_async_remote_copy(
                            src_ref=src, dst_ref=block, send_sem=send_sem.at[a, n, h, kind],
                            recv_sem=landed, device_id={"ep": target},
                            device_id_type=pl.DeviceIdType.MESH)
                        cp.start()
                        pending.append(cp)
                    arrivals.append((a, n, h, slice_of(a, base + 1 - core, h)))
    for a, n, h, block in arrivals:
        pltpu.make_async_remote_copy(
            src_ref=block, dst_ref=block, send_sem=send_sem.at[a, n, h, 0],
            recv_sem=pair_recv.at[a, n, h], device_id={"ep": other},
            device_id_type=pl.DeviceIdType.MESH).wait_recv()
    for cp in pending:
        cp.wait_send()
    keep.wait()


def gather_tokens(x, u):
    ep = lax.axis_size("ep")
    outer = 4 if ep % 8 == 0 else 1
    grid = (outer, ep // (2 * outer), 2)
    toks, width = x.shape
    spots = ep // 2
    out = jax.ShapeDtypeStruct((ep, toks, width), x.dtype)
    return pl.pallas_call(
        functools.partial(gather_kernel, grid, lax.axis_size("section")),
        out_shape=(out, out),
        in_specs=[pl.BlockSpec(memory_space=pl.ANY)] * 2,
        out_specs=(pl.BlockSpec(memory_space=pl.ANY),) * 2,
        scratch_shapes=[
            pltpu.SemaphoreType.DMA,
            pltpu.SemaphoreType.DMA((2,)),
            pltpu.SemaphoreType.DMA((2, spots, 2, 3)),
            pltpu.SemaphoreType.DMA((2, spots, 2)),
            pltpu.SemaphoreType.DMA((2, spots, 2)),
        ],
        compiler_params=pltpu.CompilerParams(collective_id=0, has_side_effects=True),
        name="gather_tokens",
    )(x, u)


def body(inputs, upstream, gate_saved, expert_ids, route_weights, w_up, w_down):
    ep = lax.axis_size("ep")
    local = w_up.shape[1]
    experts = local * ep
    toks, top = expert_ids.shape[1:]
    cap = 3 * toks * top // (2 * experts)
    width = inputs.shape[2]
    ff = w_up.shape[3]

    routing = jnp.concatenate([expert_ids[0].astype(F32), route_weights[0]], axis=1)
    routing_all = lax.all_gather(routing, "ep", axis=0, tiled=False)

    ids = expert_ids[0]
    hit = ids[:, :, None] == jnp.arange(experts, dtype=jnp.int32)
    member = jnp.any(hit, axis=1).astype(BF16)
    lower = (jnp.arange(toks)[:, None] > jnp.arange(toks)[None, :]).astype(BF16)
    rank = jnp.dot(lower, member, preferred_element_type=F32)
    place = jnp.sum(jnp.where(hit, rank[:, None, :], 0.0), axis=2)
    slot = (ids * cap + place.astype(jnp.int32)).reshape(1, toks * top)
    pick = (jnp.arange(experts * cap, dtype=jnp.int32)[:, None] == slot).astype(BF16)
    gate_send = jnp.dot(pick, gate_saved[0].reshape(toks * top, ff), preferred_element_type=F32)
    gate_send = gate_send.astype(BF16).reshape(ep, local, cap, ff)
    gate_recv = lax.all_to_all(gate_send, "ep", split_axis=0, concat_axis=0, tiled=True)

    x_all, c_all = gather_tokens(inputs[0], upstream[0])
    x_all = x_all.reshape(ep * toks, width)
    c_all = c_all.reshape(ep * toks, width)

    me = lax.axis_index("ep")
    named, weights = routing_all[:, :, :top], routing_all[:, :, top:]
    hiddens, grads = [], []
    for e in range(local):
        hits = named == (me * local + e).astype(F32)
        weight = jnp.sum(jnp.where(hits, weights, 0.0), axis=2)
        here = jnp.any(hits, axis=2)
        rank_here = lax.dot_general(here.astype(BF16), lower, (((1,), (1,)), ((), ())), preferred_element_type=F32)
        rank_here = jnp.where(here, rank_here, -1.0)
        spread = (rank_here[:, :, None] == jnp.arange(cap).astype(F32)).astype(BF16)
        gate = lax.dot_general(
            spread, gate_recv[:, e], (((2,), (1,)), ((0,), (0,))), preferred_element_type=F32
        ).reshape(ep * toks, ff)
        act = jax.nn.silu(gate) * weight.reshape(ep * toks, 1)
        u = jnp.dot(x_all, w_up[0, e], preferred_element_type=F32)
        h = lax.dot_general(c_all, w_down[0, e], (((1,), (1,)), ((), ())), preferred_element_type=F32)
        hiddens.append((act * u).astype(BF16))
        grads.append((act * h).astype(BF16))
    g = jnp.concatenate(grads, axis=1)
    up_cat = jnp.concatenate([w_up[0, e] for e in range(local)], axis=1)
    part = lax.dot_general(g, up_cat, (((1,), (1,)), ((), ())), preferred_element_type=F32)
    grad = lax.psum_scatter(part.astype(BF16), "ep", scatter_dimension=0, tiled=True)
    delivered = from_behind(grad[None], "section", -1)
    over_tokens = (((0,), (0,)), ((), ()))
    grad_up = [lax.dot_general(x_all, r, over_tokens, preferred_element_type=F32).astype(BF16) for r in grads]
    grad_down = [lax.dot_general(r, c_all, over_tokens, preferred_element_type=F32).astype(BF16) for r in hiddens]
    return (delivered, jnp.stack(grad_up)[None], jnp.stack(grad_down)[None])


def solution(mesh):
    return jax.shard_map(
        body,
        mesh=mesh,
        in_specs=(
            P("section", "ep", None),
            P("section", "ep", None),
            P("section", "ep", None, None),
            P("section", "ep", None),
            P("section", "ep", None),
            P("section", "ep", None, None),
            P("section", "ep", None, None),
        ),
        out_specs=(
            P("section", "ep", None),
            P("section", "ep", None, None),
            P("section", "ep", None, None),
        ),
        check_vma=False,
    )
```
